32 devices in a mesh: dp: 2 (over x), tp: 4 (over z), sp: 4 (over y, core).
Axes of the slice: x: 2, y: 2, z: 4, core: 2. Of those that a mesh axis runs over, the one named last changes fastest.
Arguments:
- tokens: bfloat16 [96, 1024, 768], P('dp', 'sp'), parts along dimension 0
- attn_gain: float32 [768], replicated
- w_qkv: bfloat16 [768, 3, 12, 64], P(None, None, 'tp')
- w_rel: bfloat16 [768, 12, 64], P(None, 'tp')
- bias_u: float32 [12, 64], P('tp')
- bias_v: float32 [12, 64], P('tp')
- rel_table: bfloat16 [1024, 768], replicated
- w_out: bfloat16 [12, 64, 768], P('tp')
- ffn_gain: float32 [768], replicated
- w_up: bfloat16 [768, 3072], P(None, 'tp')
- w_down: bfloat16 [3072, 768], P('tp')
Outputs:
- output 1: bfloat16 [96, 1024, 768], P('dp', 'sp'), parts along dimension 0
- output 2: bfloat16 [96, 12, 1024, 64], P(('dp', 'sp'), 'tp'), parts along dimension 0
- output 3: bfloat16 [96, 12, 1024, 64], P(('dp', 'sp'), 'tp'), parts along dimension 0
There are 2 independent parts. The reference program is written for one: setup_inputs(seed, part) draws one part's arguments, and reference() takes and returns one part's arrays. A program takes and returns all parts, laid end to end along the dimension named above; an argument that names none is the same for every part.
All inputs are finite; a program needn't handle non-finite values.
Results may differ from the reference program's by a relative error of at most 0.0122429.
Values are sent between devices in bfloat16 or wider.
A program may use at most 1 GiB of HBM per device.

```python
import jax
import jax.numpy as jnp
from jax import lax

BATCH = 48
SEQ_LEN = 1024
D_MODEL = 768
HEADS = 12
HEAD_DIM = 64
FF_DIM = 3072
QUERY_BLOCK = 128


def rms_norm(values, gain):
    vals_f32 = values.astype(jnp.float32)
    inv_rms = lax.rsqrt(jnp.mean(vals_f32 * vals_f32, axis=-1, keepdims=True) + 1e-6)
    return (vals_f32 * inv_rms * gain).astype(jnp.bfloat16)


def setup_inputs(seed: int = 0, part: int = 0) -> dict:
    key_list = jax.random.split(jax.random.key(seed), 11)
    inner_dim = HEADS * HEAD_DIM
    tokens = jax.random.normal(jax.random.fold_in(key_list[0], part), (BATCH, SEQ_LEN, D_MODEL), jnp.float32)
    attn_gain = 1.0 + 0.25 * jax.random.normal(key_list[1], (D_MODEL,), jnp.float32)
    qkv_scale = jnp.array([1.5, 1.0, 1.0], jnp.float32)[None, :, None, None] * D_MODEL ** -0.5
    w_qkv = jax.random.normal(key_list[2], (D_MODEL, 3, HEADS, HEAD_DIM), jnp.float32) * qkv_scale
    w_rel = jax.random.normal(key_list[3], (D_MODEL, HEADS, HEAD_DIM), jnp.float32) * D_MODEL ** -0.5
    bias_u = jax.random.normal(key_list[4], (HEADS, HEAD_DIM), jnp.float32)
    bias_v = jax.random.normal(key_list[5], (HEADS, HEAD_DIM), jnp.float32)
    rel_table = jax.random.normal(key_list[6], (SEQ_LEN, D_MODEL), jnp.float32)
    w_out = jax.random.normal(key_list[7], (HEADS, HEAD_DIM, D_MODEL), jnp.float32) * inner_dim ** -0.5
    ffn_gain = 1.0 + 0.25 * jax.random.normal(key_list[8], (D_MODEL,), jnp.float32)
    w_up = jax.random.normal(key_list[9], (D_MODEL, FF_DIM), jnp.float32) * D_MODEL ** -0.5
    w_down = jax.random.normal(key_list[10], (FF_DIM, D_MODEL), jnp.float32) * FF_DIM ** -0.5
    return {'tokens': tokens.astype(jnp.bfloat16), 'attn_gain': attn_gain, 'w_qkv': w_qkv.astype(jnp.bfloat16), 'w_rel': w_rel.astype(jnp.bfloat16), 'bias_u': bias_u, 'bias_v': bias_v, 'rel_table': rel_table.astype(jnp.bfloat16), 'w_out': w_out.astype(jnp.bfloat16), 'ffn_gain': ffn_gain, 'w_up': w_up.astype(jnp.bfloat16), 'w_down': w_down.astype(jnp.bfloat16)}


def block_attention(qu_blk, qv_blk, key_rows, val_rows, prev_pad, q_start):
    n_q = qu_blk.shape[1]
    win_len = SEQ_LEN + n_q
    window = lax.dynamic_slice_in_dim(prev_pad, SEQ_LEN - q_start - n_q, win_len, axis=1)
    content = jnp.einsum('hqe,hke->hqk', qu_blk.astype(jnp.float32), key_rows.astype(jnp.float32))
    pos_raw = jnp.einsum('hqe,hle->hql', qv_blk.astype(jnp.float32), window.astype(jnp.float32))
    pos_flat = pos_raw.reshape(HEADS, n_q * win_len)
    pos_term = pos_flat[:, n_q - 1:n_q - 1 + n_q * (win_len - 1)].reshape(HEADS, n_q, win_len - 1)[:, :, :SEQ_LEN]
    scores = (content + pos_term) * HEAD_DIM ** -0.5
    causal = jnp.arange(SEQ_LEN)[None, :] <= (q_start + jnp.arange(n_q))[:, None]
    scores = jnp.where(causal[None], scores, -1e30)
    exp_scores = jnp.exp(scores - jnp.max(scores, axis=-1, keepdims=True))
    row_sum = jnp.sum(exp_scores, axis=-1, keepdims=True)
    weighted = jnp.einsum('hqk,hke->hqe', exp_scores.astype(jnp.bfloat16).astype(jnp.float32), val_rows.astype(jnp.float32))
    return (weighted / row_sum).astype(jnp.bfloat16)


def reference(tokens, attn_gain, w_qkv, w_rel, bias_u, bias_v, rel_table, w_out, ffn_gain, w_up, w_down):
    rel_pos = jnp.einsum('sd,dhe->hse', rel_table.astype(jnp.float32), w_rel.astype(jnp.float32)).astype(jnp.bfloat16)
    prev_pad = jnp.concatenate([jnp.flip(rel_pos, axis=1), jnp.zeros_like(rel_pos)], axis=1)
    qkv_f32 = w_qkv.astype(jnp.float32)
    out_f32 = w_out.astype(jnp.float32)
    block_starts = jnp.arange(SEQ_LEN // QUERY_BLOCK) * QUERY_BLOCK

    def one_prompt(prompt):
        normed = rms_norm(prompt, attn_gain)
        qkv = jnp.einsum('sd,dche->chse', normed.astype(jnp.float32), qkv_f32).astype(jnp.bfloat16)
        query_rows = qkv[0].astype(jnp.float32)
        q_u = (query_rows + bias_u[:, None, :]).astype(jnp.bfloat16)
        q_v = (query_rows + bias_v[:, None, :]).astype(jnp.bfloat16)

        def one_block(q_start):
            qu_blk = lax.dynamic_slice_in_dim(q_u, q_start, QUERY_BLOCK, axis=1)
            qv_blk = lax.dynamic_slice_in_dim(q_v, q_start, QUERY_BLOCK, axis=1)
            return block_attention(qu_blk, qv_blk, qkv[1], qkv[2], prev_pad, q_start)

        blocks = lax.map(one_block, block_starts)
        attn_proj = jnp.einsum('bhqe,hed->bqd', blocks.astype(jnp.float32), out_f32)
        attn_proj = attn_proj.reshape(SEQ_LEN, D_MODEL).astype(jnp.bfloat16)
        hidden = (prompt.astype(jnp.float32) + attn_proj.astype(jnp.float32)).astype(jnp.bfloat16)
        normed_ffn = rms_norm(hidden, ffn_gain)
        up_proj = jax.nn.gelu(jnp.dot(normed_ffn, w_up, preferred_element_type=jnp.float32)).astype(jnp.bfloat16)
        down_proj = jnp.dot(up_proj, w_down, preferred_element_type=jnp.float32).astype(jnp.bfloat16)
        hidden_out = (hidden.astype(jnp.float32) + down_proj.astype(jnp.float32)).astype(jnp.bfloat16)
        return hidden_out, qkv[1], qkv[2]

    hidden_out, k_cache, v_cache = lax.map(one_prompt, tokens)
    return hidden_out, k_cache, v_cache
```

```python
import functools
import math

import jax
import jax.numpy as jnp
from jax import lax
from jax.experimental import pallas as pl
from jax.experimental.pallas import tpu as pltpu
from jax.sharding import PartitionSpec as P

BF = jnp.bfloat16
F32 = jnp.float32
HBM = pl.BlockSpec(memory_space=pltpu.HBM)
VMEM = pl.BlockSpec(memory_space=pltpu.VMEM)
TILE = 128


def chunk_sizes(own):
    return (1, 1, 2, 2, 2, 2, 2) if own == 12 else (1,) * own


def cost(flops, nbytes):
    return pl.CostEstimate(flops=int(flops), bytes_accessed=int(nbytes), transcendentals=0)


def params(mib):
    return pltpu.CompilerParams(dimension_semantics=("arbitrary",), vmem_limit_bytes=mib * 2**20)


def rms(vals, gain):
    inv = lax.rsqrt(jnp.mean(vals * vals, axis=-1, keepdims=True) + 1e-6)
    return (vals * inv * gain).astype(BF)


def proj_kernel(count, sp_ref, x_ref, gain_ref, w_ref, *rest):
    outs, buf, sem = rest[:4], rest[4], rest[5]
    step = pl.program_id(0)
    slot = lax.rem(step, 2)

    def copies(idx, sl, act):
        for part in range(4):
            @pl.when(idx == part)
            def _():
                act(pltpu.make_async_copy(buf.at[sl], outs[3 - part], sem.at[sl]))

    @pl.when(step > 1)
    def _():
        copies(step - 2, slot, lambda c: c.wait())

    for i in range(count):
        normed = rms(x_ref[i].astype(F32), gain_ref[...])
        prod = lax.dot_general(w_ref[...], normed, (((1,), (1,)), ((), ())), preferred_element_type=F32)
        buf[slot, i] = prod.astype(BF)
    copies(step, slot, lambda c: c.start())

    @pl.when(step == 3)
    def _():
        copies(step - 1, 1 - slot, lambda c: c.wait())
        copies(step, slot, lambda c: c.wait())


def project(sp, tokens, gain, w_t, off, count, own):
    rows, d_model = w_t.shape
    blk = tokens.shape[1]
    shape = jax.ShapeDtypeStruct((count, rows, blk), BF)

    def x_map(step, sp_ref):
        return ((lax.bitwise_xor(sp_ref[0], 3 - step) * own + off) // count, 0, 0)

    return pl.pallas_call(
        functools.partial(proj_kernel, count),
        out_shape=[shape] * 4,
        grid_spec=pltpu.PrefetchScalarGridSpec(
            num_scalar_prefetch=1, grid=(4,),
            in_specs=[pl.BlockSpec((count, blk, d_model), x_map), VMEM, VMEM],
            out_specs=[HBM] * 4,
            scratch_shapes=[pltpu.VMEM((2, count, rows, blk), BF), pltpu.SemaphoreType.DMA((2,))]),
        compiler_params=params(24),
        cost_estimate=cost(4 * count * 2.0 * rows * blk * d_model, 4 * count * blk * (d_model + rows) * 2),
        name="project",
    )(sp, tokens, gain, w_t)


def attend_head(h, scr, slot, table, bias_u, bias_v, o_scr, qu_scr, qv_scr, hd, seq):
    scale = F32(math.log2(math.e) * hd ** -0.5)
    row = pl.multiple_of(h * hd, hd)
    k_row = pl.multiple_of((3 + h) * hd, hd)
    v_row = pl.multiple_of((6 + h) * hd, hd)
    query = scr[slot, pl.ds(row, hd), :].astype(F32).T
    qu_scr[...] = (query + bias_u[h]).astype(BF)
    qv_scr[...] = (query + bias_v[h]).astype(BF)
    lane = lax.broadcasted_iota(jnp.int32, (TILE, TILE), 1)
    tri = lane <= lax.broadcasted_iota(jnp.int32, (TILE, TILE), 0)
    for i in range(seq // TILE):
        width = (i + 1) * TILE
        rows = slice(i * TILE, width)
        content = jnp.dot(qu_scr[rows, :], scr[slot, pl.ds(k_row, hd), :width], preferred_element_type=F32)
        raw = jnp.dot(qv_scr[rows, :], table[pl.ds(row, hd), seq - width:], preferred_element_type=F32)
        turned = [pltpu.roll(raw[:, t * TILE:(t + 1) * TILE], 1, axis=1, stride=1, stride_axis=0) for t in range(i + 1)]
        scores = []
        for t in range(i + 1):
            part = content[:, t * TILE:(t + 1) * TILE]
            if t < i:
                scores.append(part + jnp.where(tri, turned[t], turned[t + 1]))
            else:
                scores.append(jnp.where(tri, part + turned[t], F32(-1e30)))
        top = jnp.max(functools.reduce(jnp.maximum, scores), axis=1, keepdims=True)
        exps = [jnp.exp2((s - top) * scale) for s in scores]
        total = jnp.sum(functools.reduce(jnp.add, exps).T, axis=0, keepdims=True)
        probs = jnp.concatenate([e.astype(BF) for e in exps], axis=1)
        out = lax.dot_general(scr[slot, pl.ds(v_row, hd), :width], probs, (((1,), (1,)), ((), ())),
                              preferred_element_type=F32)
        o_scr[slot, pl.ds(row, hd), rows] = (out / total).astype(BF)


def attend_kernel(count, hd, seq, blk, off, sp_ref, p0, p1, p2, p3, table, bias_u, bias_v, *rest):
    k_out, v_out, o0, o1, o2, o3, scr, o_scr, qu_scr, qv_scr, in_sem, c_sem, o_sem = rest[-13:]
    sp = sp_ref[0]
    p = pl.program_id(0)
    slot = lax.rem(p, 2)
    width = 3 * hd

    def place(part):
        return pl.ds(pl.multiple_of(lax.bitwise_xor(sp, part) * blk, blk), blk)

    def in_copies(i, sl):
        return [pltpu.make_async_copy(src.at[i], scr.at[sl, :, place(r)], in_sem.at[sl])
                for r, src in enumerate((p0, p1, p2, p3))]

    def c_copies(i, sl):
        return [pltpu.make_async_copy(scr.at[sl, pl.ds((n + 1) * width, width), :], dst.at[off + i], c_sem.at[sl])
                for n, dst in enumerate((k_out, v_out))]

    def o_copies(i, sl):
        return [pltpu.make_async_copy(o_scr.at[sl, :, place(r)], dst.at[i], o_sem.at[sl])
                for r, dst in enumerate((o0, o1, o2, o3))]

    def start(copies):
        for c in copies:
            c.start()

    def wait(copies):
        for c in copies:
            c.wait()

    @pl.when(p == 0)
    def _():
        start(in_copies(p, slot))

    wait(in_copies(p, slot))
    start(c_copies(p, slot))

    @pl.when(p > 0)
    def _():
        wait(c_copies(p - 1, 1 - slot))

    @pl.when(p + 1 < count)
    def _():
        start(in_copies(p + 1, 1 - slot))

    @pl.when(p > 1)
    def _():
        wait(o_copies(p - 2, slot))

    def head(h, carry):
        attend_head(h, scr, slot, table, bias_u, bias_v, o_scr, qu_scr, qv_scr, hd, seq)
        return carry

    lax.fori_loop(0, 3, head, 0)
    start(o_copies(p, slot))

    @pl.when(p == count - 1)
    def _():
        wait(c_copies(p, slot))
        wait(o_copies(p, slot))
        if count > 1:
            wait(o_copies(p - 1, 1 - slot))


def attend(sp, pieces, table, bias_u, bias_v, k_cache, v_cache, off, own):
    count, rows, blk = pieces[0].shape
    hd = rows // 9
    seq = 4 * blk
    args = [sp, *pieces, table, bias_u, bias_v]
    in_specs = [HBM] * 4 + [VMEM] * 3
    alias = {}
    if k_cache is not None:
        args += [k_cache, v_cache]
        in_specs += [HBM, HBM]
        alias = {8: 0, 9: 1}
    c_shape = jax.ShapeDtypeStruct((own, 3 * hd, seq), BF)
    o_shape = jax.ShapeDtypeStruct((count, 3 * hd, blk), BF)
    out = pl.pallas_call(
        functools.partial(attend_kernel, count, hd, seq, blk, off),
        out_shape=[c_shape] * 2 + [o_shape] * 4,
        grid_spec=pltpu.PrefetchScalarGridSpec(
            num_scalar_prefetch=1, grid=(count,), in_specs=in_specs, out_specs=[HBM] * 6,
            scratch_shapes=[
                pltpu.VMEM((2, rows, seq), BF), pltpu.VMEM((2, 3 * hd, seq), BF),
                pltpu.VMEM((seq, hd), BF), pltpu.VMEM((seq, hd), BF),
                pltpu.SemaphoreType.DMA((2,)), pltpu.SemaphoreType.DMA((2,)), pltpu.SemaphoreType.DMA((2,))]),
        input_output_aliases=alias,
        compiler_params=params(32),
        cost_estimate=cost(count * 9e9, count * 4 * rows * blk * 4),
        name="attend",
    )(*args)
    return out[0], out[1], out[2:]


def ffn_kernel(tp, sp_ref, dev_ref, heads_ref, x_ref, gain_ref, w0, w1, w2, w3, *rest):
    y_ref, up_scr, down_scr, out_scr, sem = rest[-5:]
    d_model = x_ref.shape[-1]
    up_rows = up_scr.shape[1] // 4
    out_rows = out_scr.shape[1] // 4

    def copies():
        out = []
        for part, src in enumerate((w0, w1, w2, w3)):
            quarter = lax.bitwise_xor(dev_ref[0], part)
            r1 = pl.ds(pl.multiple_of(quarter * up_rows, up_rows), up_rows)
            r2 = pl.ds(pl.multiple_of(quarter * out_rows, out_rows), out_rows)
            out.append(pltpu.make_async_copy(src.at[:, pl.ds(2 * up_rows, out_rows), :], out_scr.at[:, r2, :], sem))
            out.append(pltpu.make_async_copy(src.at[:, pl.ds(0, up_rows), :], up_scr.at[:, r1, :], sem))
            out.append(pltpu.make_async_copy(src.at[:, pl.ds(up_rows, up_rows), :], down_scr.at[:, r1, :], sem))
        return out

    @pl.when((pl.program_id(0) == 0) & (pl.program_id(1) == 0))
    def _():
        cps = copies()
        for c in cps:
            c.start()
        for c in cps:
            c.wait()

    w_out = out_scr[...].reshape(tp * out_scr.shape[1], d_model)
    for i in range(x_ref.shape[0]):
        heads = heads_ref[:, 0, i].reshape(w_out.shape[0], x_ref.shape[1])
        attn = lax.dot_general(heads, w_out, (((0,), (0,)), ((), ())), preferred_element_type=F32).astype(BF)
        hidden = (x_ref[i].astype(F32) + attn.astype(F32)).astype(BF)
        normed = rms(hidden.astype(F32), gain_ref[...])
        acc = None
        for t in range(tp):
            up = jnp.dot(normed, up_scr[t], preferred_element_type=F32)
            act = jax.nn.gelu(up, approximate=True).astype(BF)
            down = jnp.dot(act, down_scr[t], preferred_element_type=F32)
            acc = down if acc is None else acc + down
        y_ref[i] = (hidden.astype(F32) + acc.astype(BF).astype(F32)).astype(BF)


def feed_forward(sp, dev, heads, tokens, gain, weights, y, off, own):
    tp, _, count, rows, blk = heads.shape
    d_model = tokens.shape[-1]
    step = 2 if count % 2 == 0 else 1

    def x_map(r, j, sp_ref, dev_ref):
        return ((lax.bitwise_xor(sp_ref[0], r) * own + off) // step + j, 0, 0)

    x_spec = pl.BlockSpec((step, blk, d_model), x_map)
    in_specs = [pl.BlockSpec((tp, 1, step, rows, blk), lambda r, j, *_: (0, r, j, 0, 0)), x_spec, VMEM] + [HBM] * 4
    args = [sp, dev, heads, tokens, gain, *weights]
    alias = {}
    if y is not None:
        args.append(y)
        in_specs.append(HBM)
        alias = {9: 0}
    quarter = weights[0].shape[1]
    up_rows = d_model // 4
    out_rows = quarter - 2 * up_rows
    return pl.pallas_call(
        functools.partial(ffn_kernel, tp),
        out_shape=jax.ShapeDtypeStruct(tokens.shape, BF),
        grid_spec=pltpu.PrefetchScalarGridSpec(
            num_scalar_prefetch=2, grid=(4, count // step), in_specs=in_specs, out_specs=x_spec,
            scratch_shapes=[
                pltpu.VMEM((tp, 4 * up_rows, d_model), BF), pltpu.VMEM((tp, 4 * up_rows, d_model), BF),
                pltpu.VMEM((tp, 4 * out_rows, d_model), BF), pltpu.SemaphoreType.DMA]),
        input_output_aliases=alias,
        compiler_params=pltpu.CompilerParams(dimension_semantics=("arbitrary",) * 2, vmem_limit_bytes=48 * 2**20),
        cost_estimate=cost(4 * count * blk * 2.0 * d_model * d_model * 9, 4 * count * blk * d_model * 6),
        name="feed_forward",
    )(*args)


def solution(mesh):
    n_sp, n_tp, n_dp = mesh.shape["sp"], mesh.shape["tp"], mesh.shape["dp"]

    def flip(x, axis, bit):
        size = mesh.shape[axis]
        return lax.ppermute(x, axis, [(i, i ^ bit) for i in range(size)]) if size > 1 else x

    def local_layer(tokens, attn_gain, w_qkv, w_rel, bias_u, bias_v, rel_table, w_out, ffn_gain, w_up, w_down):
        prompts, blk, d_model = tokens.shape
        n_heads, hd = bias_u.shape
        own = prompts // n_sp
        seq = n_sp * blk
        sp_idx = lax.axis_index("sp")
        quarter = (lax.axis_index("dp") % 2) * 2 + sp_idx % 2
        sp = sp_idx.astype(jnp.int32).reshape(1)
        dev = quarter.astype(jnp.int32).reshape(1)

        w_local = jnp.concatenate([
            lax.dynamic_slice_in_dim(w, quarter * (w.shape[0] // 4), w.shape[0] // 4, axis=0)
            for w in (w_up, w_down, w_out.reshape(n_heads * hd, d_model))], axis=0)
        w_own = lax.all_gather(w_local, "tp", axis=0)
        w_x = flip(w_own, "dp", 1)
        weights = (w_own, flip(w_own, "sp", 1), w_x, flip(w_x, "sp", 1))

        w_t = w_qkv.transpose(1, 2, 3, 0).reshape(3 * n_heads * hd, d_model)
        rel_t = w_rel.transpose(1, 2, 0).reshape(n_heads * hd, d_model)
        table = lax.dot_general(rel_t, jnp.flip(rel_table, axis=0), (((1,), (1,)), ((), ())),
                                preferred_element_type=F32).astype(BF)
        gain_1 = attn_gain.reshape(1, d_model)
        gain_2 = ffn_gain.reshape(1, d_model)
        u = bias_u.reshape(n_heads, 1, hd)
        v = bias_v.reshape(n_heads, 1, hd)

        k_cache = v_cache = y = None
        off = 0
        for count in chunk_sizes(own):
            mine = project(sp, tokens, gain_1, w_t, off, count, own)
            pieces = [mine[0]] + [flip(mine[r], "sp", r) for r in (1, 2, 3)]
            k_cache, v_cache, o = attend(sp, pieces, table, u, v, k_cache, v_cache, off, own)
            heads = jnp.stack([o[0]] + [flip(o[r], "sp", r) for r in (1, 2, 3)])
            heads = lax.all_gather(heads, "tp", axis=0)
            y = feed_forward(sp, dev, heads, tokens, gain_2, weights, y, off, own)
            off += count

        def as_cache(c):
            return c.reshape(own, n_heads, hd, seq).transpose(0, 1, 3, 2)

        return y, as_cache(k_cache), as_cache(v_cache)

    seq_spec = P("dp", "sp", None)
    cache_spec = P(("dp", "sp"), "tp", None, None)
    in_specs = (seq_spec, P(None), P(None, None, "tp", None), P(None, "tp", None), P("tp", None), P("tp", None),
                P(None, None), P("tp", None, None), P(None), P(None, "tp"), P("tp", None))
    return jax.shard_map(local_layer, mesh=mesh, in_specs=in_specs, out_specs=(seq_spec, cache_spec, cache_spec),
                         check_vma=False)
```

```python
import functools
import itertools
import math

import jax
import jax.numpy as jnp
from jax import lax
from jax.experimental import pallas as pl
from jax.experimental.pallas import tpu as pltpu
from jax.sharding import PartitionSpec as P


BF = jnp.bfloat16
F32 = jnp.float32
HBM = pl.BlockSpec(memory_space=pltpu.HBM)
VMEM = pl.BlockSpec(memory_space=pltpu.VMEM)
TILE = 128
VMEM_BYTES = 66_000_000
TICK = jax.ShapeDtypeStruct((8, 128), F32)
ORDER = (0, 2, 4, 6, 7, 5, 3, 1)


def chunk_sizes(own):
    return (1, 1, 2, 4, 2, 1, 1) if own == 12 else (1,) * own


def plan(n):
    lead, lag = 2, 2
    steps = [("project", i) for i in range(min(lead, n))]
    for i in range(n + lag):
        if i < n:
            steps.append(("attend", i))
        if i + lead < n:
            steps.append(("project", i + lead))
        if i < n:
            steps.append(("gather", i))
        if i == min(1, n - 1):
            steps.append(("weights", i))
        if i >= lag:
            steps.append(("feed", i - lag))
    return steps


def cost(flops, nbytes):
    return pl.CostEstimate(flops=int(flops), bytes_accessed=int(nbytes), transcendentals=0)


def params(dims):
    return pltpu.CompilerParams(dimension_semantics=("arbitrary",) * dims, vmem_limit_bytes=VMEM_BYTES)


def rms(vals, gain):
    inv = lax.rsqrt(jnp.mean(vals * vals, axis=-1, keepdims=True) + 1e-6)
    return (vals * inv * gain).astype(BF)


def proj_kernel(count, sp_ref, x_ref, gain_ref, w_ref, tick_ref, *rest):
    outs, buf, sem = rest[:4], rest[5], rest[6]
    step = pl.program_id(0)
    slot = lax.rem(step, 2)

    def copies(idx, sl, act):
        for part in range(4):
            @pl.when(idx == part)
            def _():
                act(pltpu.make_async_copy(buf.at[sl], outs[3 - part], sem.at[sl]))

    @pl.when(step > 1)
    def _():
        copies(step - 2, slot, lambda c: c.wait())

    for i in range(count):
        normed = rms(x_ref[i].astype(F32), gain_ref[...])
        prod = lax.dot_general(w_ref[...], normed, (((1,), (1,)), ((), ())), preferred_element_type=F32)
        buf[slot, i] = prod.astype(BF)
    copies(step, slot, lambda c: c.start())

    @pl.when(step == 3)
    def _():
        copies(step - 1, 1 - slot, lambda c: c.wait())
        copies(step, slot, lambda c: c.wait())


def project(sp, tokens, gain, w_t, tick, off, count, own):
    rows, d_model = w_t.shape
    blk = tokens.shape[1]
    shape = jax.ShapeDtypeStruct((count, rows, blk), BF)

    def x_map(step, sp_ref):
        return ((lax.bitwise_xor(sp_ref[0], 3 - step) * own + off) // count, 0, 0)

    return pl.pallas_call(
        functools.partial(proj_kernel, count),
        out_shape=[shape] * 4 + [TICK],
        grid_spec=pltpu.PrefetchScalarGridSpec(
            num_scalar_prefetch=1, grid=(4,),
            in_specs=[pl.BlockSpec((count, blk, d_model), x_map), VMEM, VMEM, HBM],
            out_specs=[HBM] * 5,
            scratch_shapes=[pltpu.VMEM((2, count, rows, blk), BF), pltpu.SemaphoreType.DMA((2,))]),
        compiler_params=params(1),
        cost_estimate=cost(4 * count * 2.0 * rows * blk * d_model, 4 * count * blk * (d_model + rows) * 2),
        name="project",
    )(sp, tokens, gain, w_t, tick)


def attend_head(h, scr, slot, table, bias_u, bias_v, o_scr, r_scr, c_scr, s_scr, hd, seq):
    scale = F32(math.log2(math.e) * hd ** -0.5)
    row = pl.multiple_of(h * hd, hd)
    k_row = pl.multiple_of((3 + h) * hd, hd)
    v_row = pl.multiple_of((6 + h) * hd, hd)
    lane = lax.broadcasted_iota(jnp.int32, (TILE, TILE), 1)
    tri = lane <= lax.broadcasted_iota(jnp.int32, (TILE, TILE), 0)
    step = 2 * TILE

    def multiply(i, buf):
        width = (i + 1) * TILE
        query = scr[slot, pl.ds(row, hd), i * TILE:width].T.astype(F32)
        qu = (query + bias_u[h]).astype(BF)
        qv = (query + bias_v[h]).astype(BF)
        for c in reversed(range(0, width, step)):
            end = min(width, c + step)
            r_scr[buf, :, c:end] = jnp.dot(qv, table[pl.ds(row, hd), seq - width + c:seq - width + end],
                                           preferred_element_type=F32)
            c_scr[buf, :, c:end] = jnp.dot(qu, scr[slot, pl.ds(k_row, hd), c:end], preferred_element_type=F32)
            yield

    def score(i, buf, box):
        after = None
        tops = None
        for t in reversed(range(i + 1)):
            lanes = slice(t * TILE, (t + 1) * TILE)
            turned = pltpu.roll(r_scr[buf, :, lanes], 1, axis=1, stride=1, stride_axis=0)
            if after is None:
                part = jnp.where(tri, c_scr[buf, :, lanes] + turned, F32(-1e30))
            else:
                part = c_scr[buf, :, lanes] + jnp.where(tri, turned, after)
            after = turned
            s_scr[buf, :, lanes] = part
            tops = part if tops is None else jnp.maximum(tops, part)
            if t % 2 == 0:
                yield
        box.append(jnp.max(tops, axis=1, keepdims=True))

    def combine(i, buf, box):
        width = (i + 1) * TILE
        total = None
        out = None
        top = box[-1] if len(box) == 1 else box.pop(0)
        for c in range(0, width, step):
            end = min(width, c + step)
            probs = []
            for t in range((end - c) // TILE):
                e = jnp.exp2((s_scr[buf, :, c + t * TILE:c + (t + 1) * TILE] - top) * scale)
                total = e if total is None else total + e
                probs.append(e.astype(BF))
            part = lax.dot_general(scr[slot, pl.ds(v_row, hd), c:end], jnp.concatenate(probs, axis=1),
                                   (((1,), (1,)), ((), ())), preferred_element_type=F32)
            out = part if out is None else out + part
            yield
        total = jnp.sum(total.T, axis=0, keepdims=True)
        o_scr[slot, pl.ds(row, hd), i * TILE:width] = (out / total).astype(BF)

    order = ORDER
    tops = {n: [] for n in range(len(order))}
    for n in range(len(order) + 2):
        work = []
        if n < len(order):
            work.append(multiply(order[n], n % 2))
        if 0 <= n - 1 < len(order):
            work.append(score(order[n - 1], (n - 1) % 2, tops[n - 1]))
        if 0 <= n - 2 < len(order):
            work.append(combine(order[n - 2], (n - 2) % 2, tops[n - 2]))
        for _ in itertools.zip_longest(*work):
            pass


def attend_kernel(count, hd, seq, blk, off, sp_ref, p0, p1, p2, p3, table, bias_u, bias_v, tick_ref, *rest):
    k_out, v_out, o0, o1, o2, o3, tick_out, scr, o_scr, r_scr, c_scr, s_scr, in_sem, c_sem, o_sem = rest[-15:]
    sp = sp_ref[0]
    p = pl.program_id(0)
    slot = lax.rem(p, 2)
    width = 3 * hd

    def place(part):
        return pl.ds(pl.multiple_of(lax.bitwise_xor(sp, part) * blk, blk), blk)

    def in_copies(i, sl):
        return [pltpu.make_async_copy(src.at[i], scr.at[sl, :, place(r)], in_sem.at[sl])
                for r, src in enumerate((p0, p1, p2, p3))]

    def c_copies(i, sl):
        return [pltpu.make_async_copy(scr.at[sl, pl.ds((n + 1) * width, width), :], dst.at[off + i], c_sem.at[sl])
                for n, dst in enumerate((k_out, v_out))]

    def o_copies(i, sl):
        return [pltpu.make_async_copy(o_scr.at[sl, :, place(r)], dst.at[i], o_sem.at[sl])
                for r, dst in enumerate((o0, o1, o2, o3))]

    def start(copies):
        for c in copies:
            c.start()

    def wait(copies):
        for c in copies:
            c.wait()

    @pl.when(p == 0)
    def _():
        start(in_copies(p, slot))

    wait(in_copies(p, slot))
    start(c_copies(p, slot))

    @pl.when(p > 0)
    def _():
        wait(c_copies(p - 1, 1 - slot))

    @pl.when(p + 1 < count)
    def _():
        start(in_copies(p + 1, 1 - slot))

    @pl.when(p > 1)
    def _():
        wait(o_copies(p - 2, slot))

    def head(h, carry):
        attend_head(h, scr, slot, table, bias_u, bias_v, o_scr, r_scr, c_scr, s_scr, hd, seq)
        return carry

    lax.fori_loop(0, 3, head, 0)
    start(o_copies(p, slot))

    @pl.when(p == count - 1)
    def _():
        wait(c_copies(p, slot))
        wait(o_copies(p, slot))
        if count > 1:
            wait(o_copies(p - 1, 1 - slot))


def attend(sp, pieces, table, bias_u, bias_v, tick, k_cache, v_cache, off, own):
    count, rows, blk = pieces[0].shape
    hd = rows // 9
    seq = 4 * blk
    args = [sp, *pieces, table, bias_u, bias_v, tick]
    in_specs = [HBM] * 4 + [VMEM] * 3 + [HBM]
    alias = {}
    if k_cache is not None:
        args += [k_cache, v_cache]
        in_specs += [HBM, HBM]
        alias = {9: 0, 10: 1}
    c_shape = jax.ShapeDtypeStruct((own, 3 * hd, seq), BF)
    o_shape = jax.ShapeDtypeStruct((count, 3 * hd, blk), BF)
    out = pl.pallas_call(
        functools.partial(attend_kernel, count, hd, seq, blk, off),
        out_shape=[c_shape] * 2 + [o_shape] * 4 + [TICK],
        grid_spec=pltpu.PrefetchScalarGridSpec(
            num_scalar_prefetch=1, grid=(count,), in_specs=in_specs, out_specs=[HBM] * 7,
            scratch_shapes=[
                pltpu.VMEM((2, rows, seq), BF), pltpu.VMEM((2, 3 * hd, seq), BF),
                *[pltpu.VMEM((2, TILE, seq), F32)] * 3,
                pltpu.SemaphoreType.DMA((2,)), pltpu.SemaphoreType.DMA((2,)), pltpu.SemaphoreType.DMA((2,))]),
        input_output_aliases=alias,
        compiler_params=params(1),
        cost_estimate=cost(count * 9e9, count * 4 * rows * blk * 4),
        name="attend",
    )(*args)
    return out[0], out[1], out[2:6], out[6]


def ffn_kernel(tp, sp_ref, dev_ref, heads_ref, x_ref, gain_ref, w0, w1, w2, w3, tick_ref, *rest):
    y_ref, tick_out, up_scr, down_scr, out_scr, sem = rest[-6:]
    d_model = x_ref.shape[-1]
    up_rows = up_scr.shape[1] // 4
    out_rows = out_scr.shape[1] // 4

    def copies():
        out = []
        for part, src in enumerate((w0, w1, w2, w3)):
            quarter = lax.bitwise_xor(dev_ref[0], part)
            r1 = pl.ds(pl.multiple_of(quarter * up_rows, up_rows), up_rows)
            r2 = pl.ds(pl.multiple_of(quarter * out_rows, out_rows), out_rows)
            out.append(pltpu.make_async_copy(src.at[:, pl.ds(2 * up_rows, out_rows), :], out_scr.at[:, r2, :], sem))
            out.append(pltpu.make_async_copy(src.at[:, pl.ds(0, up_rows), :], up_scr.at[:, r1, :], sem))
            out.append(pltpu.make_async_copy(src.at[:, pl.ds(up_rows, up_rows), :], down_scr.at[:, r1, :], sem))
        return out

    @pl.when((pl.program_id(0) == 0) & (pl.program_id(1) == 0))
    def _():
        cps = copies()
        for c in cps:
            c.start()
        for c in cps:
            c.wait()

    w_out = out_scr[...].reshape(tp * out_scr.shape[1], d_model)
    for i in range(x_ref.shape[0]):
        heads = heads_ref[:, 0, i].reshape(w_out.shape[0], x_ref.shape[1])
        attn = lax.dot_general(heads, w_out, (((0,), (0,)), ((), ())), preferred_element_type=F32).astype(BF)
        hidden = (x_ref[i].astype(F32) + attn.astype(F32)).astype(BF)
        normed = rms(hidden.astype(F32), gain_ref[...])
        acc = None
        for t in range(tp):
            up = jnp.dot(normed, up_scr[t], preferred_element_type=F32)
            act = jax.nn.gelu(up, approximate=True).astype(BF)
            down = jnp.dot(act, down_scr[t], preferred_element_type=F32)
            acc = down if acc is None else acc + down
        y_ref[i] = (hidden.astype(F32) + acc.astype(BF).astype(F32)).astype(BF)


def feed_forward(sp, dev, heads, tokens, gain, weights, tick, y, off, own):
    tp, _, count, rows, blk = heads.shape
    d_model = tokens.shape[-1]
    step = 2 if count % 2 == 0 else 1

    def x_map(r, j, sp_ref, dev_ref):
        return ((lax.bitwise_xor(sp_ref[0], r) * own + off) // step + j, 0, 0)

    x_spec = pl.BlockSpec((step, blk, d_model), x_map)
    in_specs = [pl.BlockSpec((tp, 1, step, rows, blk), lambda r, j, *_: (0, r, j, 0, 0)), x_spec, VMEM] + [HBM] * 5
    args = [sp, dev, heads, tokens, gain, *weights, tick]
    alias = {}
    if y is not None:
        args.append(y)
        in_specs.append(HBM)
        alias = {10: 0}
    quarter = weights[0].shape[1]
    up_rows = d_model // 4
    out_rows = quarter - 2 * up_rows
    return pl.pallas_call(
        functools.partial(ffn_kernel, tp),
        out_shape=[jax.ShapeDtypeStruct(tokens.shape, BF), TICK],
        grid_spec=pltpu.PrefetchScalarGridSpec(
            num_scalar_prefetch=2, grid=(4, count // step), in_specs=in_specs, out_specs=[x_spec, HBM],
            scratch_shapes=[
                pltpu.VMEM((tp, 4 * up_rows, d_model), BF), pltpu.VMEM((tp, 4 * up_rows, d_model), BF),
                pltpu.VMEM((tp, 4 * out_rows, d_model), BF), pltpu.SemaphoreType.DMA]),
        input_output_aliases=alias,
        compiler_params=params(2),
        cost_estimate=cost(4 * count * blk * 2.0 * d_model * d_model * 9, 4 * count * blk * d_model * 6),
        name="feed_forward",
    )(*args)


def solution(mesh):
    n_sp, n_tp, n_dp = mesh.shape["sp"], mesh.shape["tp"], mesh.shape["dp"]

    def flip(x, axis, bit):
        size = mesh.shape[axis]
        return lax.ppermute(x, axis, [(i, i ^ bit) for i in range(size)]) if size > 1 else x

    def local_layer(tokens, attn_gain, w_qkv, w_rel, bias_u, bias_v, rel_table, w_out, ffn_gain, w_up, w_down):
        prompts, blk, d_model = tokens.shape
        n_heads, hd = bias_u.shape
        own = prompts // n_sp
        seq = n_sp * blk
        sp_idx = lax.axis_index("sp")
        quarter = (lax.axis_index("dp") % 2) * 2 + sp_idx % 2
        sp = sp_idx.astype(jnp.int32).reshape(1)
        dev = quarter.astype(jnp.int32).reshape(1)

        w_local = jnp.concatenate([
            lax.dynamic_slice_in_dim(w, quarter * (w.shape[0] // 4), w.shape[0] // 4, axis=0)
            for w in (w_up, w_down, w_out.reshape(n_heads * hd, d_model))], axis=0)
        w_own = lax.all_gather(w_local, "tp", axis=0)

        w_t = w_qkv.transpose(1, 2, 3, 0).reshape(3 * n_heads * hd, d_model)
        rel_t = w_rel.transpose(1, 2, 0).reshape(n_heads * hd, d_model)
        rel_pos = lax.dot_general(rel_t, rel_table, (((1,), (1,)), ((), ())), preferred_element_type=F32).astype(BF)
        at = jnp.arange(seq)
        mirror = (at[:, None] + at[None, :] == seq - 1).astype(BF)
        table = jnp.dot(rel_pos, mirror, preferred_element_type=F32).astype(BF)
        gain_1 = attn_gain.reshape(1, d_model)
        gain_2 = ffn_gain.reshape(1, d_model)
        u = bias_u.reshape(n_heads, 1, hd)
        v = bias_v.reshape(n_heads, 1, hd)

        counts = chunk_sizes(own)
        offs = [sum(counts[:i]) for i in range(len(counts))]
        tick = jnp.zeros(TICK.shape, F32)
        k_cache = v_cache = y = None
        pieces, outs, heads = {}, {}, {}
        for kind, i in plan(len(counts)):
            if kind == "project":
                *mine, tick = project(sp, tokens, gain_1, w_t, tick, offs[i], counts[i], own)
                pieces[i] = [mine[0]] + [flip(mine[r], "sp", r) for r in (1, 2, 3)]
            elif kind == "attend":
                k_cache, v_cache, o, tick = attend(sp, pieces[i], table, u, v, tick, k_cache, v_cache, offs[i], own)
                outs[i] = [o[0]] + [flip(o[r], "sp", r) for r in (1, 2, 3)]
            elif kind == "gather":
                whole, tick = lax.optimization_barrier((jnp.stack(outs[i]), tick))
                heads[i] = lax.all_gather(whole, "tp", axis=0)
            elif kind == "weights":
                w_own, tick = lax.optimization_barrier((w_own, tick))
                w_x = flip(w_own, "dp", 1)
                weights = (w_own, flip(w_own, "sp", 1), w_x, flip(w_x, "sp", 1))
            else:
                y, tick = feed_forward(sp, dev, heads[i], tokens, gain_2, weights, tick, y, offs[i], own)

        def as_cache(c):
            return c.reshape(own, n_heads, hd, seq).transpose(0, 1, 3, 2)

        return y, as_cache(k_cache), as_cache(v_cache)

    seq_spec = P("dp", "sp", None)
    cache_spec = P(("dp", "sp"), "tp", None, None)
    in_specs = (seq_spec, P(None), P(None, None, "tp", None), P(None, "tp", None), P("tp", None), P("tp", None),
                P(None, None), P("tp", None, None), P(None), P(None, "tp"), P("tp", None))
    return jax.shard_map(local_layer, mesh=mesh, in_specs=in_specs, out_specs=(seq_spec, cache_spec, cache_spec),
                         check_vma=False)
```

```python
import functools
import itertools
import math

import jax
import jax.numpy as jnp
from jax import lax
from jax.experimental import pallas as pl
from jax.experimental.pallas import tpu as pltpu
from jax.sharding import PartitionSpec as P


BF = jnp.bfloat16
F32 = jnp.float32
HBM = pl.BlockSpec(memory_space=pltpu.HBM)
VMEM = pl.BlockSpec(memory_space=pltpu.VMEM)
TILE = 128
VMEM_BYTES = 66_000_000
TICK = jax.ShapeDtypeStruct((8, 128), F32)
ORDER = (3, 2, 1, 0)


def chunk_sizes(own):
    return (2, 3, 4, 2, 1) if own == 12 else (1,) * own


def plan(n):
    steps = [("project", (0,)), ("send", 0)]
    if n > 1:
        steps += [("project", (1,)), ("send", 1)]
    lag = 2
    for i in range(n + lag):
        if i < n:
            steps.append(("attend", i))
        if i == 0 and n > 2:
            steps.append(("project", tuple(range(2, n))))
        if 2 <= i + 1 < n:
            steps.append(("send", i + 1))
        if i == min(1, n - 1):
            steps.append(("weights", 0))
        if i == lag:
            steps.append(("weights", 1))
        if i >= lag:
            steps.append(("feed", i - lag))
        if i < n:
            steps.append(("gather", i))
    return steps


def cost(flops, nbytes):
    return pl.CostEstimate(flops=int(flops), bytes_accessed=int(nbytes), transcendentals=0)


def params(dims):
    return pltpu.CompilerParams(dimension_semantics=("arbitrary",) * dims, vmem_limit_bytes=VMEM_BYTES)


def rms(vals, gain):
    inv = lax.rsqrt(jnp.mean(vals * vals, axis=-1, keepdims=True) + 1e-6)
    return (vals * inv * gain).astype(BF)


def proj_kernel(counts, sp_ref, x_ref, gain_ref, w_ref, tick_ref, *rest):
    outs, buf, sem = rest[:-3], rest[-2], rest[-1]
    step = pl.program_id(0)
    slot = lax.rem(step, 2)
    total = pl.num_programs(0)

    def copies(idx, sl, act):
        first = 0
        for n, count in enumerate(counts):
            for part in range(4):
                @pl.when((idx >= first) & (idx < first + count))
                def _(first=first, n=n, part=part):
                    act(pltpu.make_async_copy(buf.at[sl], outs[4 * n + 3 - part].at[idx - first], sem.at[sl]))

                first += count

    @pl.when(step > 1)
    def _():
        copies(step - 2, slot, lambda c: c.wait())

    normed = rms(x_ref[0].astype(F32), gain_ref[...])
    prod = lax.dot_general(w_ref[...], normed, (((1,), (1,)), ((), ())), preferred_element_type=F32)
    buf[slot] = prod.astype(BF)
    copies(step, slot, lambda c: c.start())

    @pl.when(step == total - 1)
    def _():
        copies(step - 1, 1 - slot, lambda c: c.wait())
        copies(step, slot, lambda c: c.wait())


def project(sp, tokens, gain, w_t, tick, offs, counts, own):
    rows, d_model = w_t.shape
    blk = tokens.shape[1]

    def x_map(step, sp_ref):
        base = jnp.int32(0)
        first = 0
        for off, count in zip(offs, counts):
            for part in range(4):
                here = lax.bitwise_xor(sp_ref[0], 3 - part) * own + off + step - first
                base = jnp.where(step >= first, here, base)
                first += count
        return base, 0, 0

    out = pl.pallas_call(
        functools.partial(proj_kernel, counts),
        out_shape=[jax.ShapeDtypeStruct((n, rows, blk), BF) for n in counts for _ in range(4)] + [TICK],
        grid_spec=pltpu.PrefetchScalarGridSpec(
            num_scalar_prefetch=1, grid=(4 * sum(counts),),
            in_specs=[pl.BlockSpec((1, blk, d_model), x_map), VMEM, VMEM, HBM],
            out_specs=[HBM] * (4 * len(counts) + 1),
            scratch_shapes=[pltpu.VMEM((2, rows, blk), BF), pltpu.SemaphoreType.DMA((2,))]),
        compiler_params=params(1),
        cost_estimate=cost(4 * sum(counts) * 2.0 * rows * blk * d_model, 4 * sum(counts) * blk * (d_model + rows) * 2),
        name="project",
    )(sp, tokens, gain, w_t, tick)
    return [out[4 * n:4 * n + 4] for n in range(len(counts))], out[-1]


def attend_heads(heads, scr, slot, table, bias_u, bias_v, o_scr, r_scr, c_scr, s_scr, hd, seq):
    scale = F32(math.log2(math.e) * hd ** -0.5)
    lane = lax.broadcasted_iota(jnp.int32, (TILE, TILE), 1)
    tri = lane <= lax.broadcasted_iota(jnp.int32, (TILE, TILE), 0)
    step = 2 * TILE
    tiles = seq // TILE

    def parts(pair):
        return (pair, 0), (tiles - 1 - pair, (pair + 1) * TILE)

    def multiply(h, pair, buf):
        for i, base in parts(pair):
            width = (i + 1) * TILE
            query = scr[slot, h * hd:(h + 1) * hd, i * TILE:width].T.astype(F32)
            qu = (query + bias_u[h]).astype(BF)
            qv = (query + bias_v[h]).astype(BF)
            for c in reversed(range(0, width, step)):
                end = min(width, c + step)
                r_scr[buf, :, base + c:base + end] = jnp.dot(
                    qv, table[h * hd:(h + 1) * hd, seq - width + c:seq - width + end], preferred_element_type=F32)
                c_scr[buf, :, base + c:base + end] = jnp.dot(
                    qu, scr[slot, (3 + h) * hd:(4 + h) * hd, c:end], preferred_element_type=F32)
                yield

    def score(h, pair, buf, box):
        for i, base in parts(pair):
            after = None
            tops = None
            for t in reversed(range(i + 1)):
                lanes = slice(base + t * TILE, base + (t + 1) * TILE)
                turned = pltpu.roll(r_scr[buf, :, lanes], 1, axis=1, stride=1, stride_axis=0)
                if after is None:
                    part = jnp.where(tri, c_scr[buf, :, lanes] + turned, F32(-1e30))
                else:
                    part = c_scr[buf, :, lanes] + jnp.where(tri, turned, after)
                after = turned
                s_scr[buf, :, lanes] = part
                tops = part if tops is None else jnp.maximum(tops, part)
                if t % 2 == 0:
                    yield
            box.append(jnp.max(tops, axis=1, keepdims=True))

    def combine(h, pair, buf, box):
        for n, (i, base) in enumerate(parts(pair)):
            width = (i + 1) * TILE
            total = None
            out = None
            for c in range(0, width, step):
                end = min(width, c + step)
                probs = []
                for t in range(c // TILE, end // TILE):
                    e = jnp.exp2((s_scr[buf, :, base + t * TILE:base + (t + 1) * TILE] - box[n]) * scale)
                    total = e if total is None else total + e
                    probs.append(e.astype(BF))
                part = lax.dot_general(scr[slot, (6 + h) * hd:(7 + h) * hd, c:end], jnp.concatenate(probs, axis=1),
                                       (((1,), (1,)), ((), ())), preferred_element_type=F32)
                out = part if out is None else out + part
                yield
            total = jnp.sum(total.T, axis=0, keepdims=True)
            o_scr[slot, h * hd:(h + 1) * hd, i * TILE:width] = (out / total).astype(BF)

    items = [(h, pair) for h in heads for pair in ORDER]
    tops = [[] for _ in items]
    for n in range(len(items) + 2):
        work = []
        if 0 <= n - 2 < len(items):
            work.append(combine(*items[n - 2], (n - 2) % 2, tops[n - 2]))
        if 0 <= n - 1 < len(items):
            work.append(score(*items[n - 1], (n - 1) % 2, tops[n - 1]))
        if n < len(items):
            work.append(multiply(*items[n], n % 2))
        for _ in itertools.zip_longest(*work):
            pass


def attend_kernel(count, hd, seq, blk, off, sp_ref, p0, p1, p2, p3, table, bias_u, bias_v, tick_ref, *rest):
    k_out, v_out, o0, o1, o2, o3, _, scr, o_scr, r_scr, c_scr, s_scr, in_sem, c_sem, o_sem = rest[-15:]
    sp = sp_ref[0]
    p = pl.program_id(0)
    slot = lax.rem(p, 2)
    width = 3 * hd

    def place(part):
        return pl.ds(pl.multiple_of(lax.bitwise_xor(sp, part) * blk, blk), blk)

    def in_copies(i, sl):
        return [pltpu.make_async_copy(src.at[i], scr.at[sl, :, place(r)], in_sem.at[sl])
                for r, src in enumerate((p0, p1, p2, p3))]

    def c_copies(i, sl):
        return [pltpu.make_async_copy(scr.at[sl, pl.ds((n + 1) * width, width), :], dst.at[off + i], c_sem.at[sl])
                for n, dst in enumerate((k_out, v_out))]

    def o_copies(i, sl):
        return [pltpu.make_async_copy(o_scr.at[sl, :, place(r)], dst.at[i], o_sem.at[sl])
                for r, dst in enumerate((o0, o1, o2, o3))]

    def start(copies):
        for c in copies:
            c.start()

    def wait(copies):
        for c in copies:
            c.wait()

    @pl.when(p == 0)
    def _():
        start(in_copies(p, slot))

    wait(in_copies(p, slot))
    start(c_copies(p, slot))

    @pl.when(p > 0)
    def _():
        wait(c_copies(p - 1, 1 - slot))

    @pl.when(p + 1 < count)
    def _():
        start(in_copies(p + 1, 1 - slot))

    @pl.when(p > 1)
    def _():
        wait(o_copies(p - 2, slot))

    attend_heads(range(3), scr, slot, table, bias_u, bias_v, o_scr, r_scr, c_scr, s_scr, hd, seq)
    start(o_copies(p, slot))

    @pl.when(p == count - 1)
    def _():
        wait(c_copies(p, slot))
        wait(o_copies(p, slot))
        if count > 1:
            wait(o_copies(p - 1, 1 - slot))


def attend(sp, pieces, table, bias_u, bias_v, tick, k_cache, v_cache, off, own):
    count, rows, blk = pieces[0].shape
    hd = rows // 9
    seq = 4 * blk
    args = [sp, *pieces, table, bias_u, bias_v, tick]
    in_specs = [HBM] * 4 + [VMEM] * 3 + [HBM]
    alias = {}
    if k_cache is not None:
        args += [k_cache, v_cache]
        in_specs += [HBM, HBM]
        alias = {9: 0, 10: 1}
    c_shape = jax.ShapeDtypeStruct((own, 3 * hd, seq), BF)
    o_shape = jax.ShapeDtypeStruct((count, 3 * hd, blk), BF)
    out = pl.pallas_call(
        functools.partial(attend_kernel, count, hd, seq, blk, off),
        out_shape=[c_shape] * 2 + [o_shape] * 4 + [TICK],
        grid_spec=pltpu.PrefetchScalarGridSpec(
            num_scalar_prefetch=1, grid=(count,), in_specs=in_specs, out_specs=[HBM] * 7,
            scratch_shapes=[
                pltpu.VMEM((2, rows, seq), BF), pltpu.VMEM((2, 3 * hd, seq), BF),
                *[pltpu.VMEM((2, TILE, seq + TILE), F32)] * 3,
                pltpu.SemaphoreType.DMA((2,)), pltpu.SemaphoreType.DMA((2,)), pltpu.SemaphoreType.DMA((2,))]),
        input_output_aliases=alias,
        compiler_params=params(1),
        cost_estimate=cost(count * 9e9, count * 4 * rows * blk * 4),
        name="attend",
    )(*args)
    return out[0], out[1], out[2:6], out[6]


def gelu(x):
    half = 0.5 * x
    inner = x * (F32(math.sqrt(2 / math.pi)) + F32(0.044715 * math.sqrt(2 / math.pi)) * (x * x))
    return (half + half * jnp.tanh(inner)).astype(BF)


def ffn_kernel(tp, sp_ref, dev_ref, heads_ref, x_ref, gain_ref, w0, w1, w2, w3, tick_ref, *rest):
    y_ref, _, up_scr, down_scr, out_scr, sem = rest[-6:]
    d_model = x_ref.shape[-1]
    up_rows = up_scr.shape[1] // 4
    out_rows = out_scr.shape[1] // 4

    def copies():
        out = []
        for part, src in enumerate((w0, w1, w2, w3)):
            quarter = lax.bitwise_xor(dev_ref[0], part)
            r1 = pl.ds(pl.multiple_of(quarter * up_rows, up_rows), up_rows)
            r2 = pl.ds(pl.multiple_of(quarter * out_rows, out_rows), out_rows)
            out.append(pltpu.make_async_copy(src.at[:, pl.ds(2 * up_rows, out_rows), :], out_scr.at[:, r2, :], sem))
            out.append(pltpu.make_async_copy(src.at[:, pl.ds(0, up_rows), :], up_scr.at[:, r1, :], sem))
            out.append(pltpu.make_async_copy(src.at[:, pl.ds(up_rows, up_rows), :], down_scr.at[:, r1, :], sem))
        return out

    @pl.when((pl.program_id(0) == 0) & (pl.program_id(1) == 0))
    def _():
        cps = copies()
        for c in cps:
            c.start()
        for c in cps:
            c.wait()

    w_out = out_scr[...].reshape(tp * out_scr.shape[1], d_model)
    ready = []
    for i in range(x_ref.shape[0]):
        heads = heads_ref[:, 0, i].reshape(w_out.shape[0], x_ref.shape[1])
        attn = lax.dot_general(heads, w_out, (((0,), (0,)), ((), ())), preferred_element_type=F32).astype(BF)
        hidden = (x_ref[i].astype(F32) + attn.astype(F32)).astype(BF)
        ready.append((hidden, rms(hidden.astype(F32), gain_ref[...])))
    for i, (hidden, normed) in enumerate(ready):
        acc = None
        for t in range(tp):
            up = gelu(jnp.dot(normed, up_scr[t], preferred_element_type=F32))
            down = jnp.dot(up, down_scr[t], preferred_element_type=F32)
            acc = down if acc is None else acc + down
        y_ref[i] = (hidden.astype(F32) + acc.astype(BF).astype(F32)).astype(BF)


def feed_forward(sp, dev, heads, tokens, gain, weights, tick, y, off, own):
    tp, _, count, rows, blk = heads.shape
    d_model = tokens.shape[-1]
    step = 2 if count % 2 == 0 else count

    def x_map(r, j, sp_ref, dev_ref):
        return lax.bitwise_xor(sp_ref[0], r) * own + off + j * step, 0, 0

    x_spec = pl.BlockSpec((pl.Element(step), pl.Element(blk), pl.Element(d_model)), x_map)
    in_specs = [pl.BlockSpec((tp, 1, step, rows, blk), lambda r, j, *_: (0, r, j, 0, 0)), x_spec, VMEM] + [HBM] * 5
    args = [sp, dev, heads, tokens, gain, *weights, tick]
    alias = {}
    if y is not None:
        args.append(y)
        in_specs.append(HBM)
        alias = {10: 0}
    quarter = weights[0].shape[1]
    up_rows = d_model // 4
    out_rows = quarter - 2 * up_rows
    return pl.pallas_call(
        functools.partial(ffn_kernel, tp),
        out_shape=[jax.ShapeDtypeStruct(tokens.shape, BF), TICK],
        grid_spec=pltpu.PrefetchScalarGridSpec(
            num_scalar_prefetch=2, grid=(4, count // step), in_specs=in_specs, out_specs=[x_spec, HBM],
            scratch_shapes=[
                pltpu.VMEM((tp, 4 * up_rows, d_model), BF), pltpu.VMEM((tp, 4 * up_rows, d_model), BF),
                pltpu.VMEM((tp, 4 * out_rows, d_model), BF), pltpu.SemaphoreType.DMA]),
        input_output_aliases=alias,
        compiler_params=params(2),
        cost_estimate=cost(4 * count * blk * 2.0 * d_model * d_model * 9, 4 * count * blk * d_model * 6),
        name="feed_forward",
    )(*args)


def solution(mesh):
    n_sp = mesh.shape["sp"]

    def flip(x, axis, bit):
        size = mesh.shape[axis]
        return lax.ppermute(x, axis, [(i, i ^ bit) for i in range(size)]) if size > 1 else x

    def layer(tokens, attn_gain, w_qkv, w_rel, bias_u, bias_v, rel_table, w_out, ffn_gain, w_up, w_down):
        prompts, blk, d_model = tokens.shape
        n_heads, hd = bias_u.shape
        own = prompts // n_sp
        seq = n_sp * blk
        sp_idx = lax.axis_index("sp")
        quarter = (lax.axis_index("dp") % 2) * 2 + sp_idx % 2
        sp = sp_idx.astype(jnp.int32).reshape(1)
        dev = quarter.astype(jnp.int32).reshape(1)

        w_local = jnp.concatenate([
            lax.dynamic_slice_in_dim(w, quarter * (w.shape[0] // 4), w.shape[0] // 4, axis=0)
            for w in (w_up, w_down, w_out.reshape(n_heads * hd, d_model))], axis=0)
        w_own = lax.all_gather(w_local, "tp", axis=0)

        w_t = w_qkv.transpose(1, 2, 3, 0).reshape(3 * n_heads * hd, d_model)
        rel_t = w_rel.transpose(1, 2, 0).reshape(n_heads * hd, d_model)
        rel_pos = lax.dot_general(rel_t, rel_table, (((1,), (1,)), ((), ())), preferred_element_type=F32).astype(BF)
        at = jnp.arange(seq)
        mirror = (at[:, None] + at[None, :] == seq - 1).astype(BF)
        table = jnp.dot(rel_pos, mirror, preferred_element_type=F32).astype(BF)
        gain_1 = attn_gain.reshape(1, d_model)
        gain_2 = ffn_gain.reshape(1, d_model)
        u = bias_u.reshape(n_heads, 1, hd)
        v = bias_v.reshape(n_heads, 1, hd)

        counts = chunk_sizes(own)
        offs = [sum(counts[:i]) for i in range(len(counts))]
        tick = jnp.zeros(TICK.shape, F32)
        k_cache = v_cache = y = None
        pieces, outs, heads = {}, {}, {}

        def exchange(mine):
            out = [mine[0]]
            for r in (1, 2, 3):
                out.append(flip(mine[r], "sp", r))
            return out

        for kind, i in plan(len(counts)):
            if kind == "project":
                got, tick = project(sp, tokens, gain_1, w_t, tick, tuple(offs[j] for j in i),
                                    tuple(counts[j] for j in i), own)
                pieces.update(zip(i, got))
            elif kind == "send":
                mine, tick = lax.optimization_barrier((pieces[i], tick))
                pieces[i] = exchange(mine)
            elif kind == "attend":
                k_cache, v_cache, o, tick = attend(sp, pieces[i], table, u, v, tick, k_cache, v_cache, offs[i], own)
                outs[i] = exchange(o)
            elif kind == "gather":
                mine, tick = lax.optimization_barrier((outs[i], tick))
                heads[i] = lax.all_gather(jnp.stack(mine), "tp", axis=0)
            elif kind == "weights" and i == 0:
                w_own, tick = lax.optimization_barrier((w_own, tick))
                weights = [w_own, flip(w_own, "sp", 1)]
                weights.append(flip(w_own, "dp", 1))
            elif kind == "weights":
                w_x, tick = lax.optimization_barrier((weights[2], tick))
                weights = [*weights[:2], w_x, flip(w_x, "sp", 1)]
            else:
                y, tick = feed_forward(sp, dev, heads[i], tokens, gain_2, weights, tick, y, offs[i], own)

        def as_cache(c):
            return c.reshape(own, n_heads, hd, seq).transpose(0, 1, 3, 2)

        return y, as_cache(k_cache), as_cache(v_cache)

    seq_spec = P("dp", "sp", None)
    cache_spec = P(("dp", "sp"), "tp", None, None)
    in_specs = (seq_spec, P(None), P(None, None, "tp", None), P(None, "tp", None), P("tp", None), P("tp", None),
                P(None, None), P("tp", None, None), P(None), P(None, "tp"), P("tp", None))
    return jax.shard_map(layer, mesh=mesh, in_specs=in_specs, out_specs=(seq_spec, cache_spec, cache_spec),
                         check_vma=False)
```
